32 devices in a mesh: orient: 4 (over z), slab: 8 (over y, x, core).
Axes of the slice: x: 2, y: 2, z: 4, core: 2. Of those that a mesh axis runs over, the one named last changes fastest.
Arguments:
- polarization: bfloat16 [8, 2, 3, 8, 9216], P('orient', None, None, 'slab'), may hold values from -6 to 6
- occupied: int32 [8, 9216], P('slab'), may hold values from 0 to 1, as said below
- orient_table: int32 [8, 2], replicated, may hold values from 0 to 15
- dir_index: int32 [2048, 2], replicated, may hold values from 0 to 179
Outputs:
- mueller: float32 [4, 2048], P(None, 'slab')
The draws below stay inside these ranges and needn't reach their ends.
Inputs may be any that keep to these rules, and one draw needn't show every extreme that they name: 1 marks an occupied dipole cell.
All inputs are finite; a program needn't handle non-finite values.
Results may differ from the reference program's by a relative error of at most 0.00087.
Values may be sent and summed in bfloat16 or wider, within the bound.
A program may use at most 64 MiB of HBM per device.

```python
import math
import jax
import jax.numpy as jnp
from jax import lax

GX = 96
GY = 96
DIRS = 2048
ORIENT_GRID = 16
THETA_GRID = 180
GXY = 9216
GZ = 8
ORIENTS = 8


def draw_occupied(key, part):
    first_key = jax.random.fold_in(key, 11)
    second_key = jax.random.fold_in(key, 23)
    radius = jax.random.randint(first_key, (), 3 * GX // 4, GX + 1)
    planes_iota = jnp.arange(GZ, dtype=jnp.int32)[:, None]
    cells_iota = jnp.arange(GX * GY, dtype=jnp.int32)[None, :]
    offset_x = 2 * (cells_iota % GX) + 1 - GX
    offset_y = 2 * (cells_iota // GX) + 1 - GY
    offset_z = (2 * planes_iota + 1 - GZ) * GX // GZ
    inside = offset_x * offset_x + offset_y * offset_y + offset_z * offset_z <= radius * radius
    keeper = jax.random.randint(second_key, (GZ, GX * GY), 0, 8) != 0
    return (inside & keeper).astype(jnp.int32)


def with_ends(array, own_key, least, high):
    longest = array.shape.index(max(array.shape))
    spots = []
    for shift in (0, 1):
        where = [jax.random.randint(jax.random.fold_in(own_key, axis), (), 0, length) for axis, length in enumerate(array.shape)]
        where[longest] = (where[longest] + shift) % array.shape[longest]
        spots.append(tuple(where))
    return array.at[spots[0]].set(least).at[spots[1]].set(high)


def steps_of(rng, dims, pieces, least, top_value):
    def one(axis_at, blocks):
        steps = jax.random.uniform(jax.random.fold_in(jax.random.fold_in(rng, 6), axis_at), (blocks,), jnp.float32, least / len(pieces), top_value / len(pieces))
        return jnp.repeat(jnp.exp(steps), dims[axis_at] // blocks).reshape((-1,) + (1,) * (len(dims) - axis_at - 1))

    level = one(*pieces[0])
    for cut in pieces[1:]:
        level = level * one(*cut)
    return level


def normal_values(rng, extent, scale, limit, cuts=(), held_as=jnp.bfloat16):
    factor_of = steps_of(rng, extent, cuts, -0.22, 0.18) if cuts else 1.0
    values = jax.random.normal(rng, extent, jnp.float32) * scale * factor_of
    return jnp.minimum(jnp.maximum(values, -limit), limit).astype(held_as)


def setup_inputs(seed: int = 0) -> dict:
    streams_of = jax.random.split(jax.random.key(seed), 5)
    polarization = normal_values(streams_of[0], (ORIENTS, 2, 3, GZ, GXY), 1.0, 6.0, ((0, 4), (3, 8)))
    occupied = draw_occupied(jax.random.fold_in(streams_of[4], 71), 0)
    orient_table = with_ends(jax.random.randint(streams_of[2], (ORIENTS, 2), 0, ORIENT_GRID), jax.random.fold_in(streams_of[2], 1), 0, ORIENT_GRID - 1).astype(jnp.int32)
    dir_index = with_ends(jax.random.randint(streams_of[3], (DIRS, 2), 0, THETA_GRID), jax.random.fold_in(streams_of[3], 1), 0, THETA_GRID - 1).astype(jnp.int32)
    return {"polarization": polarization, "occupied": occupied, "orient_table": orient_table, "dir_index": dir_index}


wave_step = 0.4


def direction_angles(dir_index):
    polar_angle = (dir_index[:, 0].astype(jnp.float32) + 0.5) * (math.pi / THETA_GRID)
    azimuth = dir_index[:, 1].astype(jnp.float32) * (2.0 * math.pi / THETA_GRID)
    return polar_angle, azimuth


def unit_vectors(polar_angle, azimuth):
    return (jnp.sin(polar_angle) * jnp.cos(azimuth), jnp.sin(polar_angle) * jnp.sin(azimuth), jnp.cos(polar_angle))


def phase_block(within, plane_index, normals):
    xcoord = (within % GX).astype(jnp.float32)
    ycoord = (within // GX).astype(jnp.float32)
    zcoord = plane_index.astype(jnp.float32)
    angle = wave_step * (xcoord[:, None] * normals[0][None, :] + ycoord[:, None] * normals[1][None, :] + zcoord[:, None] * normals[2][None, :])
    return jnp.concatenate([jnp.cos(angle), -jnp.sin(angle)], axis=1).astype(jnp.bfloat16)


def orient_weights(orient_table):
    turn_angle = orient_table[:, 0].astype(jnp.float32) * (2.0 * math.pi / ORIENT_GRID)
    weight = jnp.sin((orient_table[:, 1].astype(jnp.float32) + 0.5) * (math.pi / ORIENT_GRID))
    return turn_angle, weight


def mueller_sum(amplitude, orient_table, polar_angle, azimuth):
    turn_angle, weight = orient_weights(orient_table)
    relative = azimuth[None, :] - turn_angle[:, None]
    cos_polar = jnp.cos(polar_angle)[None, :]
    sin_polar = jnp.sin(polar_angle)[None, :]
    cos_turn = jnp.cos(relative)
    sin_turn = jnp.sin(relative)
    parallel = (cos_polar * cos_turn, cos_polar * sin_turn, -sin_polar)
    across = (-sin_turn, cos_turn, None)

    def project(polar_index, basis_set):
        summed = amplitude[:, polar_index, 0] * basis_set[0][:, None, :] + amplitude[:, polar_index, 1] * basis_set[1][:, None, :]
        if basis_set[2] is not None:
            summed = summed + amplitude[:, polar_index, 2] * basis_set[2][:, None, :]
        return summed

    def square(values):
        return values[:, 0] * values[:, 0] + values[:, 1] * values[:, 1]

    lower_right = project(1, across)
    upper_left = project(0, parallel)
    upper_right = project(0, across)
    lower_left = project(1, parallel)
    elem_total = 0.5 * (square(lower_right) + square(upper_left) + square(upper_right) + square(lower_left))
    elem_diff = 0.5 * (square(upper_left) - square(lower_right) + square(lower_left) - square(upper_right))
    elem_real = (lower_right[:, 0] * upper_left[:, 0] + lower_right[:, 1] * upper_left[:, 1]
                 + upper_right[:, 0] * lower_left[:, 0] + upper_right[:, 1] * lower_left[:, 1])
    elem_imag = (upper_left[:, 1] * lower_right[:, 0] - upper_left[:, 0] * lower_right[:, 1]
                 + lower_left[:, 1] * upper_right[:, 0] - lower_left[:, 0] * upper_right[:, 1])
    stacked = jnp.stack([elem_total, elem_diff, elem_real, elem_imag])
    return jnp.sum(stacked * weight[None, :, None], axis=1)


def reference(polarization, occupied, orient_table, dir_index):
    polar_angle, azimuth = direction_angles(dir_index)
    normals = unit_vectors(polar_angle, azimuth)
    masked = polarization * occupied.astype(jnp.bfloat16)[None, None, None]
    cells_all = GZ * GXY
    flattened = masked.reshape(ORIENTS * 6, cells_all)
    block_size = math.gcd(cells_all, 4096)

    def accumulate(summed, block_index):
        offset = block_index * block_size
        segment = lax.dynamic_slice_in_dim(flattened, offset, block_size, 1)
        cell_index = offset + jnp.arange(block_size, dtype=jnp.int32)
        phase = phase_block(cell_index % GXY, cell_index // GXY, normals)
        return summed + jnp.dot(segment, phase, preferred_element_type=jnp.float32), None

    initial = jnp.zeros((ORIENTS * 6, 2 * DIRS), jnp.float32)
    amplitude = lax.scan(accumulate, initial, jnp.arange(cells_all // block_size, dtype=jnp.int32))[0]
    amplitude = amplitude.reshape(ORIENTS, 2, 3, 2, DIRS)
    summed = mueller_sum(amplitude, orient_table, polar_angle, azimuth)
    weight_total = jnp.sum(orient_weights(orient_table)[1])
    return summed / (weight_total * float(GZ * GXY))
```

```python
import functools
import math

import jax
import jax.numpy as jnp
import numpy as np
from jax import lax
from jax.experimental import pallas as pl
from jax.experimental.pallas import tpu as pltpu
from jax.sharding import PartitionSpec as P

GX = 96
ORIENT_GRID = 16
THETA_GRID = 180
LANES = 128
RX = 32
RY = 24
wave_step = 0.4
MESH = pl.DeviceIdType.MESH
F32 = jnp.float32
BF16 = jnp.bfloat16
PER = LANES // math.gcd(LANES, GX)
TILES = GX // math.gcd(LANES, GX)
HALF = RX // 2
GROUPS = RY // 2 * RX // LANES


def sincos(angle):
    quarter = jnp.round(angle * (2.0 / math.pi))
    rest = angle - quarter * 1.5703125
    rest = rest - quarter * 4.83826794896619e-4
    square = rest * rest
    sine = rest + rest * square * (
        -1.6666654611e-1 + square * (8.3321608736e-3 + square * -1.9515295891e-4)
    )
    cosine = 1.0 - 0.5 * square + square * square * (
        4.166664568298827e-2
        + square * (-1.388731625493765e-3 + square * 2.443315711809948e-5)
    )
    turns = quarter.astype(jnp.int32)
    odd = (turns & 1) == 1
    sin_sign = jnp.where((turns & 2) == 2, -1.0, 1.0)
    cos_sign = jnp.where(((turns + 1) & 2) == 2, -1.0, 1.0)
    return (
        jnp.where(odd, cosine, sine) * sin_sign,
        jnp.where(odd, sine, cosine) * cos_sign,
    )


def prolate(length, count):
    band = math.cos(wave_step)
    at = np.arange(length)
    near = at[1:] * (length - at[1:]) / 2.0
    matrix = np.diag(((length - 1 - 2 * at) / 2.0) ** 2 * band) + np.diag(near, 1) + np.diag(near, -1)
    vectors = np.linalg.eigh(matrix)[1][:, ::-1][:, :count]
    middle = at - (length - 1) / 2.0
    even, odd = vectors[:, 0::2], vectors[:, 1::2]
    even = (even + even[::-1]) / 2.0
    odd = (odd - odd[::-1]) / 2.0
    even = even * np.where(even[length // 2] < 0, -1.0, 1.0)
    odd = odd * np.where(odd[length // 2] < 0, -1.0, 1.0)
    return even, odd


def split(values):
    high = np.asarray(values, np.float32).astype(jnp.bfloat16)
    low = (np.asarray(values, np.float64) - high.astype(np.float64)).astype(np.float32)
    return high, low.astype(jnp.bfloat16)


def tables(cells):
    lines = cells // GX
    tiles = cells // LANES
    even_x, odd_x = prolate(GX, RX)
    even_y, odd_y = prolate(lines, RY)
    both_y = np.stack([even_y, odd_y], axis=2).reshape(lines, RY)
    first = np.zeros((2, TILES, 2, RY, tiles, 2))
    for tile in range(tiles):
        line = tile * LANES // GX
        for next_line in range(2):
            for p in range(2):
                first[p, tile % TILES, next_line, :, tile, p] = both_y[line + next_line]
    first = first.reshape(2 * TILES * 2 * RY, tiles * 2)
    rows = np.concatenate(split(first), axis=1)
    block = np.concatenate([even_x, odd_x], axis=1)
    columns = np.concatenate(split(np.tile(block, (1, LANES // RX))), axis=0)
    pieces = []
    for even, odd in ((even_x, odd_x), (even_y, odd_y)):
        for part in (even, odd):
            length = part.shape[0]
            half = np.zeros((HALF, length // 2))
            half[: part.shape[1]] = 2.0 * part[length // 2 :].T
            pieces.append(half)
    trig = np.stack(pieces)
    high, low = split(trig)
    trig = np.concatenate([high, high, low], axis=2)
    return rows, columns, trig.reshape(4 * HALF, -1)


def high_low(values):
    high = values.astype(BF16)
    return high, (values - high.astype(F32)).astype(BF16)


def kernel(
    slab_size, orient_size, planes, cells_all,
    pol_hbm, occ_hbm, table_hbm, dirs_hbm, rows_hbm, columns_hbm, trig_hbm, out_ref,
    held_pol, held_occ, table_ref, dirs_ref, rows_ref, columns_ref, trig_ref,
    twice, coef, found, turned, vv, landed, mine, parts,
    load_sem, send_sem, recv_sem, part_send, part_recv,
):
    slab = lax.axis_index("slab")
    orient = lax.axis_index("orient")
    partner = slab + 1 - 2 * (slab % 2)
    width = dirs_ref.shape[1]
    all_orients = table_ref.shape[1]
    tiles = held_occ.shape[0] // planes
    pair_rows = 2 * tiles
    blocks = held_pol.shape[0] // (planes * pair_rows)
    orients = blocks // 3
    group = blocks * 2
    loads = [
        pltpu.make_async_copy(occ_hbm, held_occ, load_sem.at[0]),
        pltpu.make_async_copy(pol_hbm, held_pol, load_sem.at[1]),
        pltpu.make_async_copy(rows_hbm, rows_ref, load_sem.at[2]),
        pltpu.make_async_copy(columns_hbm, columns_ref, load_sem.at[3]),
        pltpu.make_async_copy(dirs_hbm.at[partner], dirs_ref, load_sem.at[4]),
        pltpu.make_async_copy(table_hbm, table_ref, load_sem.at[5]),
        pltpu.make_async_copy(trig_hbm, trig_ref, load_sem.at[6]),
    ]
    for load in loads:
        load.start()

    barrier = pltpu.get_barrier_semaphore()
    for step in range(1, slab_size):
        pl.semaphore_signal(
            barrier, inc=1, device_id=(orient, (slab + step) % slab_size),
            device_id_type=MESH,
        )
    for step in range(1, orient_size):
        pl.semaphore_signal(
            barrier, inc=1, device_id=((orient + step) % orient_size, partner),
            device_id_type=MESH,
        )

    for load in loads[:4]:
        load.wait()
    lane = lax.broadcasted_iota(jnp.int32, (1, LANES), 1)
    kept = held_occ[...].astype(F32)
    twice[pl.ds(0, planes * tiles, stride=2), :] = kept
    twice[pl.ds(1, planes * tiles, stride=2), :] = kept
    columns = [columns_ref[0:GX, :]] * PER, [columns_ref[GX : 2 * GX, :]] * PER
    columns = jnp.concatenate(columns[0] + columns[1] + columns[0], axis=0)
    step_blocks = 2 - blocks % 2
    for plane in range(planes):
        mask = twice[plane * pair_rows : (plane + 1) * pair_rows, :].astype(BF16)
        for start in range(0, blocks, step_blocks):
            masked = jnp.concatenate(
                [
                    held_pol[pl.ds(((start + i) * planes + plane) * pair_rows, pair_rows), :] * mask
                    for i in range(step_blocks)
                ],
                axis=1,
            )
            lines = jnp.dot(
                rows_ref[...], jnp.concatenate([masked, masked], axis=0),
                preferred_element_type=F32,
            )
            stacked = []
            for i in range(step_blocks):
                for p in range(2):
                    wide = []
                    for j in range(TILES):
                        base = (p * TILES + j) * 2 * RY
                        at = slice(i * LANES, (i + 1) * LANES)
                        limit = GX - j * LANES % GX
                        wide.append(
                            jnp.where(
                                lane < limit,
                                lines[base : base + RY, at],
                                lines[base + RY : base + 2 * RY, at],
                            )
                        )
                    stacked.append(jnp.concatenate(wide, axis=1))
            high, low = high_low(jnp.concatenate(stacked, axis=0))
            small = jnp.dot(
                jnp.concatenate([high, high, low], axis=1), columns,
                preferred_element_type=F32,
            )
            count = step_blocks * 2 * RY
            coef[start * 2 * RY : start * 2 * RY + count, :] = small
            coef[(blocks + start) * 2 * RY : (blocks + start) * 2 * RY + count, :] = small
        lines_of = [coef[pl.ds(ky, 2 * group, stride=RY), :] for ky in range(RY)]
        upper = lane % RX >= HALF
        is_low = lax.broadcasted_iota(jnp.int32, (2 * group, LANES), 0) >= group
        for imag in range(2):
            for g in range(GROUPS):
                whole = None
                for q in range(LANES // RX - 1, -1, -1):
                    a = g * (LANES // RX) + q
                    one, two = lines_of[2 * a + imag], lines_of[2 * a + 1 - imag]
                    block = jnp.where(upper, two, one)
                    whole = block if whole is None else jnp.where(lane < (q + 1) * RX, block, whole)
                high = whole.astype(BF16).astype(F32)
                at = (imag * GROUPS + g) * LANES
                landed[slab, plane, 0 : 2 * group, at : at + LANES] = jnp.where(
                    is_low, whole - high, high
                ).astype(BF16)

    pl.semaphore_wait(barrier, slab_size - 1 + orient_size - 1)
    order = [at + 1 - 2 * (at % 2) for at in range(slab_size)]

    def slab_copy(source, target):
        piece = landed.at[source, :, pl.ds(0, 2 * group), :]
        return pltpu.make_async_remote_copy(
            src_ref=piece,
            dst_ref=piece,
            send_sem=send_sem.at[target],
            recv_sem=recv_sem.at[source],
            device_id=(orient, target),
            device_id_type=MESH,
        )

    for target in order:
        @pl.when(slab != target)
        def _():
            slab_copy(slab, target).start()

    for load in loads[4:]:
        load.wait()
    dirs = dirs_ref[...].astype(F32)
    is_polar = lax.broadcasted_iota(jnp.int32, (2, width), 0) == 0
    angles = jnp.where(
        is_polar, (dirs + 0.5) * (math.pi / THETA_GRID), dirs * (2.0 * math.pi / THETA_GRID)
    )
    sines, cosines = sincos(angles)
    sin_p, cos_p = sines[0:1], cosines[0:1]
    sin_a, cos_a = sines[1:2], cosines[1:2]
    azimuth = angles[1:2]
    normals = (sin_p * cos_a, sin_p * sin_a)
    parts_of = []
    for axis in range(2):
        length = trig_ref.shape[1] // 3
        step = lax.broadcasted_iota(jnp.int32, (length, width), 0).astype(F32) + 0.5
        sine, cosine = sincos(step * (wave_step * normals[axis]))
        for kind, wave in enumerate((cosine, sine)):
            high, low = high_low(wave)
            at = (axis * 2 + kind) * HALF
            parts_of.append(
                jnp.dot(
                    trig_ref[at : at + HALF, :],
                    jnp.concatenate([high, low, high], axis=0),
                    preferred_element_type=F32,
                )
            )
    even_x, odd_x, even_y, odd_y = parts_of
    deep = RY // 2 * RX
    for a in range(RY // 2):
        one, two = even_y[a : a + 1], odd_y[a : a + 1]
        for kind, pieces in enumerate(
            (
                (even_x * one, -(odd_x * two)),
                (even_x * two, odd_x * one),
            )
        ):
            high, low = high_low(jnp.concatenate(pieces, axis=0))
            vv[kind, a * RX : (a + 1) * RX, :] = high
            vv[kind, deep + a * RX : deep + (a + 1) * RX, :] = low

    tilt_row = lax.broadcasted_iota(jnp.int32, (all_orients, width), 0)
    tilts = jnp.zeros((all_orients, width), F32)
    for o in range(all_orients):
        tilts = jnp.where(tilt_row == o, table_ref[1, o].astype(F32), tilts)
    weights = sincos((tilts + 0.5) * (math.pi / ORIENT_GRID))[0]
    share = 1.0 / (jnp.sum(weights, axis=0, keepdims=True) * cells_all)
    own_row = lax.broadcasted_iota(jnp.int32, (2 * orients, width), 0) % orients
    turns = jnp.zeros((2 * orients, width), F32)
    tilt = jnp.zeros((2 * orients, width), F32)
    for o in range(orients):
        turns = jnp.where(own_row == o, table_ref[0, orient * orients + o].astype(F32), turns)
        tilt = jnp.where(own_row == o, table_ref[1, orient * orients + o].astype(F32), tilt)
    sin_q, cos_q = sincos(azimuth - turns * (2.0 * math.pi / ORIENT_GRID))
    weight = sincos((tilt + 0.5) * (math.pi / ORIENT_GRID))[0] * share
    depth_at = lax.broadcasted_iota(jnp.int32, (slab_size * planes, width), 0).astype(F32)
    sin_z, cos_z = sincos(depth_at * (wave_step * cos_p))
    turned[0] = cos_z
    turned[1] = sin_z

    for source in order[::-1]:
        @pl.when(slab != source)
        def _():
            slab_copy(source, slab).wait_recv()

    space = landed.shape[2]
    everything = landed[...].reshape(slab_size * planes * space, 2 * deep)
    real_in, imag_in = everything[:, :deep], everything[:, deep:]
    real = jnp.dot(
        jnp.concatenate([real_in, real_in], axis=1), vv[0], preferred_element_type=F32
    )
    imag = jnp.dot(
        jnp.concatenate([imag_in, imag_in], axis=1), vv[1], preferred_element_type=F32
    )
    total_r = total_i = None
    for z in range(slab_size * planes):
        at = slice(z * space, z * space + 2 * group)
        c, s = turned[0, z : z + 1, :], turned[1, z : z + 1, :]
        now_r = real[at] * c - imag[at] * s
        now_i = imag[at] * c + real[at] * s
        total_r = now_r if total_r is None else total_r + now_r
        total_i = now_i if total_i is None else total_i + now_i
    total_r, total_i = total_r[:group] + total_r[group:], total_i[:group] + total_i[group:]
    piece = min(width, LANES)
    for h in range(width // piece):
        found[h, :group, :piece] = total_r[:, h * piece : (h + 1) * piece]
        found[h, group:, :piece] = total_i[:, h * piece : (h + 1) * piece]

    def entry(c, p):
        return jnp.concatenate(
            [
                found[h, pl.ds(2 * c + p, 2 * orients, stride=6), :][:, :piece]
                for h in range(width // piece)
            ],
            axis=1,
        )

    par, across = [], []
    for p in range(2):
        one, two, three = entry(0, p), entry(1, p), entry(2, p)
        par.append(cos_p * (one * cos_q + two * sin_q) - sin_p * three)
        across.append(two * cos_q - one * sin_q)
    par_square = par[0] * par[0] + par[1] * par[1]
    across_square = across[0] * across[0] + across[1] * across[1]

    def swap(values):
        return jnp.concatenate([values[orients:], -values[:orients]], axis=0)

    elements = (
        0.5 * (par_square + across_square),
        0.5 * (par_square - across_square),
        across[1] * par[0] + across[0] * par[1],
        par[0] * swap(across[1]) + par[1] * swap(across[0]),
    )
    mine[...] = jnp.concatenate(
        [jnp.sum(element * weight, axis=0, keepdims=True) for element in elements], axis=0
    )

    def part_copy(step):
        return pltpu.make_async_remote_copy(
            src_ref=mine,
            dst_ref=parts.at[orient],
            send_sem=part_send.at[step],
            recv_sem=part_recv.at[step],
            device_id=((orient + step) % orient_size, partner),
            device_id_type=MESH,
        )

    for step in range(orient_size):
        part_copy(step).start()
    for target in order:
        @pl.when(slab != target)
        def _():
            slab_copy(slab, target).wait_send()
    for step in range(orient_size):
        back = (orient + orient_size - step) % orient_size
        pltpu.make_async_remote_copy(
            src_ref=mine,
            dst_ref=parts.at[back],
            send_sem=part_send.at[step],
            recv_sem=part_recv.at[step],
            device_id=(back, partner),
            device_id_type=MESH,
        ).wait_recv()
    summed = parts[0]
    for o in range(1, orient_size):
        summed = summed + parts[o]
    out_ref[...] = summed
    for step in range(orient_size):
        part_copy(step).wait_send()


def shards(slab_size, orient_size, polarization, occupied, orient_table, dir_index):
    orients, _, components, planes, cells = polarization.shape
    group = orients * 6
    tiles = cells // LANES
    width = dir_index.shape[0] // slab_size
    pol = polarization.reshape(orients, 2, components, planes, tiles, LANES)
    pol = pol.transpose(0, 2, 3, 4, 1, 5).reshape(-1, LANES)
    occ = occupied.reshape(planes * tiles, LANES)
    dirs = dir_index.T.reshape(2, slab_size, width).transpose(1, 0, 2)
    rows, columns, trig = (jnp.asarray(table) for table in tables(cells))
    space = -(-2 * group // 16) * 16
    deep = RY // 2 * RX
    vmem = pl.BlockSpec(memory_space=pltpu.VMEM)
    anywhere = pl.BlockSpec(memory_space=pltpu.HBM)
    return pl.pallas_call(
        functools.partial(
            kernel, slab_size, orient_size, planes, float(planes * slab_size * cells)
        ),
        out_shape=pltpu.VMEM((4, width), F32),
        in_specs=[anywhere] * 7,
        out_specs=vmem,
        scratch_shapes=[
            pltpu.VMEM(pol.shape, BF16),
            pltpu.VMEM(occ.shape, jnp.int32),
            pltpu.SMEM((2, orient_table.shape[0]), jnp.int32),
            pltpu.VMEM((2, width), jnp.int32),
            pltpu.VMEM(rows.shape, BF16),
            pltpu.VMEM(columns.shape, BF16),
            pltpu.VMEM(trig.shape, BF16),
            pltpu.VMEM((planes * tiles * 2, LANES), F32),
            pltpu.VMEM((2 * group * RY, LANES), F32),
            pltpu.VMEM((max(width // LANES, 1), 2 * group, LANES), F32),
            pltpu.VMEM((2, slab_size * planes, width), F32),
            pltpu.VMEM((2, 2 * deep, width), BF16),
            pltpu.VMEM((slab_size, planes, space, 2 * deep), BF16),
            pltpu.VMEM((4, width), F32),
            pltpu.VMEM((orient_size, 4, width), F32),
            pltpu.SemaphoreType.DMA((7,)),
            pltpu.SemaphoreType.DMA((slab_size,)),
            pltpu.SemaphoreType.DMA((slab_size,)),
            pltpu.SemaphoreType.DMA((orient_size,)),
            pltpu.SemaphoreType.DMA((orient_size,)),
        ],
        compiler_params=pltpu.CompilerParams(
            collective_id=0, has_side_effects=True
        ),
    )(pol, occ, orient_table.T, dirs, rows, columns, trig)


def solution(mesh):
    return jax.shard_map(
        functools.partial(shards, mesh.shape["slab"], mesh.shape["orient"]),
        mesh=mesh,
        in_specs=(P("orient", None, None, "slab", None), P("slab", None), P(), P()),
        out_specs=P(None, "slab"),
        check_vma=False,
    )
```

```python
import functools
import math

import jax
import jax.numpy as jnp
import numpy as np
from jax import lax
from jax.experimental import pallas as pl
from jax.experimental.pallas import tpu as pltpu
from jax.sharding import PartitionSpec as P

GX = 96
ORIENT_GRID = 16
THETA_GRID = 180
LANES = 128
RX = 32
RY = 24
wave_step = 0.4
MESH = pl.DeviceIdType.MESH
F32 = jnp.float32
BF16 = jnp.bfloat16
PER = LANES // math.gcd(LANES, GX)
TILES = GX // math.gcd(LANES, GX)
HALF = RX // 2
GROUPS = RY // 2 * RX // LANES


def sincos(angle):
    quarter = jnp.round(angle * (2.0 / math.pi))
    rest = angle - quarter * 1.5703125
    rest = rest - quarter * 4.83826794896619e-4
    square = rest * rest
    sine = rest + rest * square * (
        -1.6666654611e-1 + square * (8.3321608736e-3 + square * -1.9515295891e-4)
    )
    cosine = 1.0 - 0.5 * square + square * square * (
        4.166664568298827e-2
        + square * (-1.388731625493765e-3 + square * 2.443315711809948e-5)
    )
    turns = quarter.astype(jnp.int32)
    odd = (turns & 1) == 1
    sin_sign = jnp.where((turns & 2) == 2, -1.0, 1.0)
    cos_sign = jnp.where(((turns + 1) & 2) == 2, -1.0, 1.0)
    return (
        jnp.where(odd, cosine, sine) * sin_sign,
        jnp.where(odd, sine, cosine) * cos_sign,
    )


def prolate(length, count):
    band = math.cos(wave_step)
    at = np.arange(length)
    near = at[1:] * (length - at[1:]) / 2.0
    matrix = np.diag(((length - 1 - 2 * at) / 2.0) ** 2 * band) + np.diag(near, 1) + np.diag(near, -1)
    vectors = np.linalg.eigh(matrix)[1][:, ::-1][:, :count]
    middle = at - (length - 1) / 2.0
    even, odd = vectors[:, 0::2], vectors[:, 1::2]
    even = (even + even[::-1]) / 2.0
    odd = (odd - odd[::-1]) / 2.0
    even = even * np.where(even[length // 2] < 0, -1.0, 1.0)
    odd = odd * np.where(odd[length // 2] < 0, -1.0, 1.0)
    return even, odd


def split(values):
    high = np.asarray(values, np.float32).astype(jnp.bfloat16)
    low = (np.asarray(values, np.float64) - high.astype(np.float64)).astype(np.float32)
    return high, low.astype(jnp.bfloat16)


def tables(cells):
    lines = cells // GX
    tiles = cells // LANES
    even_x, odd_x = prolate(GX, RX)
    even_y, odd_y = prolate(lines, RY)
    both_y = np.stack([even_y, odd_y], axis=2).reshape(lines, RY)
    first = np.zeros((TILES, 2, RY, tiles))
    for tile in range(tiles):
        line = tile * LANES // GX
        for next_line in range(2):
            first[tile % TILES, next_line, :, tile] = both_y[line + next_line]
    first = first.reshape(TILES * 2 * RY, tiles)
    rows = np.concatenate(split(first), axis=1)
    block = np.concatenate([even_x, odd_x], axis=1)
    columns = np.concatenate(split(np.tile(block, (1, LANES // RX))), axis=0)
    pieces = []
    for even, odd in ((even_x, odd_x), (even_y, odd_y)):
        for part in (even, odd):
            length = part.shape[0]
            half = np.zeros((HALF, length // 2))
            half[: part.shape[1]] = 2.0 * part[length // 2 :].T
            pieces.append(half)
    trig = np.stack(pieces)
    high, low = split(trig)
    trig = np.concatenate([high, high, low], axis=2)
    return rows, columns, trig.reshape(4 * HALF, -1)


def high_low(values):
    high = values.astype(BF16)
    return high, (values - high.astype(F32)).astype(BF16)


def kernel(
    slab_size, orient_size, planes, cells_all,
    pol_hbm, occ_hbm, table_hbm, dirs_hbm, rows_hbm, columns_hbm, trig_hbm, out_ref,
    held_pol, held_occ, table_ref, dirs_ref, rows_ref, columns_ref, trig_ref,
    spread, halves, coef, found, turned, vv, landed, mine, parts,
    load_sem, send_sem, recv_sem, part_send, part_recv,
):
    slab = lax.axis_index("slab")
    orient = lax.axis_index("orient")
    is_odd = slab % 2 == 1
    odd = slab + 1 - slab % 2
    width = dirs_ref.shape[2]
    both = 2 * width
    all_orients = table_ref.shape[1]
    tiles = held_occ.shape[0] // planes
    pair_rows = 2 * tiles
    blocks = held_pol.shape[0] // (planes * pair_rows)
    orients = blocks // 3
    group = blocks * 2
    loads = [
        pltpu.make_async_copy(occ_hbm, held_occ, load_sem.at[0]),
        pltpu.make_async_copy(pol_hbm, held_pol, load_sem.at[1]),
        pltpu.make_async_copy(rows_hbm, rows_ref, load_sem.at[2]),
        pltpu.make_async_copy(columns_hbm, columns_ref, load_sem.at[3]),
        pltpu.make_async_copy(dirs_hbm.at[pl.ds(odd - 1, 2)], dirs_ref, load_sem.at[4]),
        pltpu.make_async_copy(table_hbm, table_ref, load_sem.at[5]),
        pltpu.make_async_copy(trig_hbm, trig_ref, load_sem.at[6]),
    ]
    for load in loads:
        load.start()

    barrier = pltpu.get_barrier_semaphore()

    def greet(plane_of, target):
        pl.semaphore_signal(
            barrier, inc=1, device_id=(plane_of, target), device_id_type=MESH
        )

    @pl.when(is_odd)
    def _():
        for step in range(1, slab_size):
            greet(orient, (slab + step) % slab_size)

    @pl.when(jnp.logical_not(is_odd))
    def _():
        greet(orient, odd)

    for step in range(1, orient_size):
        greet((orient + step) % orient_size, odd)

    for load in loads[:4]:
        load.wait()
    lane = lax.broadcasted_iota(jnp.int32, (1, LANES), 1)
    columns = [columns_ref[0:GX, :]] * PER, [columns_ref[GX : 2 * GX, :]] * PER
    columns = jnp.concatenate(columns[0] + columns[1] + columns[0], axis=0)
    for plane in range(planes):
        kept = held_occ[plane * tiles : (plane + 1) * tiles, :].astype(F32)
        for block in range(blocks):
            at = (block * planes + plane) * pair_rows
            spread[block] = held_pol[at : at + pair_rows, :].astype(F32)
            masked = jnp.concatenate(
                [spread[block, pl.ds(p, tiles, stride=2), :] * kept for p in range(2)], axis=1
            )
            lines = jnp.dot(
                rows_ref[...], jnp.concatenate([masked, masked], axis=0).astype(BF16),
                preferred_element_type=F32,
            )
            stacked = []
            for p in range(2):
                wide = []
                for j in range(TILES):
                    base = j * 2 * RY
                    at = slice(p * LANES, (p + 1) * LANES)
                    limit = GX - j * LANES % GX
                    wide.append(
                        jnp.where(
                            lane < limit,
                            lines[base : base + RY, at],
                            lines[base + RY : base + 2 * RY, at],
                        )
                    )
                stacked.append(jnp.concatenate(wide, axis=1))
            high, low = high_low(jnp.concatenate(stacked, axis=0))
            halves[0, block * 2 * RY : (block + 1) * 2 * RY, :] = high
            halves[1, block * 2 * RY : (block + 1) * 2 * RY, :] = low
        small = jnp.dot(
            jnp.concatenate([halves[0], halves[0], halves[1]], axis=1), columns,
            preferred_element_type=F32,
        )
        coef[0 : group * RY, :] = small
        coef[group * RY : 2 * group * RY, :] = small
        lines_of = [coef[pl.ds(ky, 2 * group, stride=RY), :] for ky in range(RY)]
        upper = lane % RX >= HALF
        is_low = lax.broadcasted_iota(jnp.int32, (2 * group, LANES), 0) >= group
        for imag in range(2):
            for g in range(GROUPS):
                whole = None
                for q in range(LANES // RX - 1, -1, -1):
                    a = g * (LANES // RX) + q
                    one, two = lines_of[2 * a + imag], lines_of[2 * a + 1 - imag]
                    block = jnp.where(upper, two, one)
                    whole = block if whole is None else jnp.where(lane < (q + 1) * RX, block, whole)
                high = whole.astype(BF16).astype(F32)
                at = (imag * GROUPS + g) * LANES
                landed[slab, plane, 0 : 2 * group, at : at + LANES] = jnp.where(
                    is_low, whole - high, high
                ).astype(BF16)

    pl.semaphore_wait(barrier, slab_size // 2 + slab % 2 * (2 * orient_size - 2))
    order = list(range(1, slab_size, 2))

    def slab_copy(source, target):
        piece = landed.at[source, :, pl.ds(0, 2 * group), :]
        return pltpu.make_async_remote_copy(
            src_ref=piece,
            dst_ref=piece,
            send_sem=send_sem.at[target],
            recv_sem=recv_sem.at[source],
            device_id=(orient, target),
            device_id_type=MESH,
        )

    for target in order:
        @pl.when(slab != target)
        def _():
            slab_copy(slab, target).start()

    for load in loads[4:]:
        load.wait()

    def part_copy(step, core):
        return pltpu.make_async_remote_copy(
            src_ref=mine.at[core],
            dst_ref=parts.at[orient],
            send_sem=part_send.at[core, step],
            recv_sem=part_recv.at[step],
            device_id=((orient + step) % orient_size, odd - 1 + core),
            device_id_type=MESH,
        )

    routes = [(step, core) for step in range(orient_size - 1, -1, -1) for core in range(2) if step + 1 - core]

    @pl.when(is_odd)
    def _():
        dirs = jnp.concatenate([dirs_ref[0], dirs_ref[1]], axis=1).astype(F32)
        is_polar = lax.broadcasted_iota(jnp.int32, (2, both), 0) == 0
        angles = jnp.where(
            is_polar, (dirs + 0.5) * (math.pi / THETA_GRID), dirs * (2.0 * math.pi / THETA_GRID)
        )
        sines, cosines = sincos(angles)
        sin_p, cos_p = sines[0:1], cosines[0:1]
        sin_a, cos_a = sines[1:2], cosines[1:2]
        azimuth = angles[1:2]
        normals = (sin_p * cos_a, sin_p * sin_a)
        parts_of = []
        for axis in range(2):
            length = trig_ref.shape[1] // 3
            step = lax.broadcasted_iota(jnp.int32, (length, both), 0).astype(F32) + 0.5
            sine, cosine = sincos(step * (wave_step * normals[axis]))
            for kind, wave in enumerate((cosine, sine)):
                high, low = high_low(wave)
                at = (axis * 2 + kind) * HALF
                parts_of.append(
                    jnp.dot(
                        trig_ref[at : at + HALF, :],
                        jnp.concatenate([high, low, high], axis=0),
                        preferred_element_type=F32,
                    )
                )
        even_x, odd_x, even_y, odd_y = parts_of
        deep = RY // 2 * RX
        for a in range(RY // 2):
            one, two = even_y[a : a + 1], odd_y[a : a + 1]
            for kind, pieces in enumerate(
                (
                    (even_x * one, -(odd_x * two)),
                    (even_x * two, odd_x * one),
                )
            ):
                high, low = high_low(jnp.concatenate(pieces, axis=0))
                vv[kind, a * RX : (a + 1) * RX, :] = high
                vv[kind, deep + a * RX : deep + (a + 1) * RX, :] = low

        tilt_row = lax.broadcasted_iota(jnp.int32, (all_orients, both), 0)
        tilts = jnp.zeros((all_orients, both), F32)
        for o in range(all_orients):
            tilts = jnp.where(tilt_row == o, table_ref[1, o].astype(F32), tilts)
        weights = sincos((tilts + 0.5) * (math.pi / ORIENT_GRID))[0]
        share = 1.0 / (jnp.sum(weights, axis=0, keepdims=True) * cells_all)
        own_row = lax.broadcasted_iota(jnp.int32, (2 * orients, both), 0) % orients
        turns = jnp.zeros((2 * orients, both), F32)
        tilt = jnp.zeros((2 * orients, both), F32)
        for o in range(orients):
            turns = jnp.where(own_row == o, table_ref[0, orient * orients + o].astype(F32), turns)
            tilt = jnp.where(own_row == o, table_ref[1, orient * orients + o].astype(F32), tilt)
        sin_q, cos_q = sincos(azimuth - turns * (2.0 * math.pi / ORIENT_GRID))
        weight = sincos((tilt + 0.5) * (math.pi / ORIENT_GRID))[0] * share
        depth_at = lax.broadcasted_iota(jnp.int32, (slab_size * planes, both), 0).astype(F32)
        sin_z, cos_z = sincos(depth_at * (wave_step * cos_p))
        turned[0] = cos_z
        turned[1] = sin_z

        for source in range(slab_size - 1, -1, -1):
            @pl.when(slab != source)
            def _():
                slab_copy(source, slab).wait_recv()

        space = landed.shape[2]
        everything = landed[...].reshape(slab_size * planes * space, 2 * deep)
        real_in, imag_in = everything[:, :deep], everything[:, deep:]
        real = jnp.dot(
            jnp.concatenate([real_in, real_in], axis=1), vv[0], preferred_element_type=F32
        )
        imag = jnp.dot(
            jnp.concatenate([imag_in, imag_in], axis=1), vv[1], preferred_element_type=F32
        )
        total_r = total_i = None
        for z in range(slab_size * planes):
            at = slice(z * space, z * space + 2 * group)
            c, s = turned[0, z : z + 1, :], turned[1, z : z + 1, :]
            now_r = real[at] * c - imag[at] * s
            now_i = imag[at] * c + real[at] * s
            total_r = now_r if total_r is None else total_r + now_r
            total_i = now_i if total_i is None else total_i + now_i
        total_r, total_i = total_r[:group] + total_r[group:], total_i[:group] + total_i[group:]
        piece = min(both, LANES)
        for h in range(both // piece):
            found[h, :group, :piece] = total_r[:, h * piece : (h + 1) * piece]
            found[h, group:, :piece] = total_i[:, h * piece : (h + 1) * piece]

        def entry(c, p):
            return jnp.concatenate(
                [
                    found[h, pl.ds(2 * c + p, 2 * orients, stride=6), :][:, :piece]
                    for h in range(both // piece)
                ],
                axis=1,
            )

        par, across = [], []
        for p in range(2):
            one, two, three = entry(0, p), entry(1, p), entry(2, p)
            par.append(cos_p * (one * cos_q + two * sin_q) - sin_p * three)
            across.append(two * cos_q - one * sin_q)
        par_square = par[0] * par[0] + par[1] * par[1]
        across_square = across[0] * across[0] + across[1] * across[1]

        def swap(values):
            return jnp.concatenate([values[orients:], -values[:orients]], axis=0)

        elements = (
            0.5 * (par_square + across_square),
            0.5 * (par_square - across_square),
            across[1] * par[0] + across[0] * par[1],
            par[0] * swap(across[1]) + par[1] * swap(across[0]),
        )
        result = jnp.concatenate(
            [jnp.sum(element * weight, axis=0, keepdims=True) for element in elements], axis=0
        )
        mine[0] = result[:, :width]
        mine[1] = result[:, width:]
        parts[orient] = result[:, width:]

        for step, core in routes:
            part_copy(step, core).start()

    for target in order:
        @pl.when(slab != target)
        def _():
            slab_copy(slab, target).wait_send()

    def arrival(step):
        back = (orient + orient_size - step) % orient_size
        return pltpu.make_async_remote_copy(
            src_ref=mine.at[0],
            dst_ref=parts.at[back],
            send_sem=part_send.at[0, step],
            recv_sem=part_recv.at[step],
            device_id=(back, odd),
            device_id_type=MESH,
        )

    @pl.when(jnp.logical_not(is_odd))
    def _():
        arrival(0).wait_recv()

    for step in range(1, orient_size):
        arrival(step).wait_recv()
    summed = parts[0]
    for o in range(1, orient_size):
        summed = summed + parts[o]
    out_ref[...] = summed

    @pl.when(is_odd)
    def _():
        for step, core in routes:
            part_copy(step, core).wait_send()


def shards(slab_size, orient_size, polarization, occupied, orient_table, dir_index):
    orients, _, components, planes, cells = polarization.shape
    group = orients * 6
    tiles = cells // LANES
    width = dir_index.shape[0] // slab_size
    pol = polarization.reshape(orients, 2, components, planes, tiles, LANES)
    pol = pol.transpose(0, 2, 3, 4, 1, 5).reshape(-1, LANES)
    occ = occupied.reshape(planes * tiles, LANES)
    dirs = dir_index.T.reshape(2, slab_size, width).transpose(1, 0, 2)
    rows, columns, trig = (jnp.asarray(table) for table in tables(cells))
    space = -(-2 * group // 16) * 16
    deep = RY // 2 * RX
    vmem = pl.BlockSpec(memory_space=pltpu.VMEM)
    anywhere = pl.BlockSpec(memory_space=pltpu.HBM)
    return pl.pallas_call(
        functools.partial(
            kernel, slab_size, orient_size, planes, float(planes * slab_size * cells)
        ),
        out_shape=pltpu.VMEM((4, width), F32),
        in_specs=[anywhere] * 7,
        out_specs=vmem,
        scratch_shapes=[
            pltpu.VMEM(pol.shape, BF16),
            pltpu.VMEM(occ.shape, jnp.int32),
            pltpu.SMEM((2, orient_table.shape[0]), jnp.int32),
            pltpu.VMEM((2, 2, width), jnp.int32),
            pltpu.VMEM(rows.shape, BF16),
            pltpu.VMEM(columns.shape, BF16),
            pltpu.VMEM(trig.shape, BF16),
            pltpu.VMEM((3 * orients, tiles * 2, LANES), F32),
            pltpu.VMEM((2, group * RY, TILES * LANES), BF16),
            pltpu.VMEM((2 * group * RY, LANES), F32),
            pltpu.VMEM((max(2 * width // LANES, 1), 2 * group, LANES), F32),
            pltpu.VMEM((2, slab_size * planes, 2 * width), F32),
            pltpu.VMEM((2, 2 * deep, 2 * width), BF16),
            pltpu.VMEM((slab_size, planes, space, 2 * deep), BF16),
            pltpu.VMEM((2, 4, width), F32),
            pltpu.VMEM((orient_size, 4, width), F32),
            pltpu.SemaphoreType.DMA((7,)),
            pltpu.SemaphoreType.DMA((slab_size,)),
            pltpu.SemaphoreType.DMA((slab_size,)),
            pltpu.SemaphoreType.DMA((2, orient_size)),
            pltpu.SemaphoreType.DMA((orient_size,)),
        ],
        compiler_params=pltpu.CompilerParams(
            collective_id=0, has_side_effects=True
        ),
    )(pol, occ, orient_table.T, dirs, rows, columns, trig)


def solution(mesh):
    return jax.shard_map(
        functools.partial(shards, mesh.shape["slab"], mesh.shape["orient"]),
        mesh=mesh,
        in_specs=(P("orient", None, None, "slab", None), P("slab", None), P(), P()),
        out_specs=P(None, "slab"),
        check_vma=False,
    )
```

```python
import functools
import math

import jax
import jax.numpy as jnp
import numpy as np
from jax import lax
from jax.experimental import pallas as pl
from jax.experimental.pallas import tpu as pltpu
from jax.sharding import PartitionSpec as P

GX = 96
ORIENT_GRID = 16
THETA_GRID = 180
LANES = 128
RX = 32
RY = 24
wave_step = 0.4
MESH = pl.DeviceIdType.MESH
F32 = jnp.float32
BF16 = jnp.bfloat16
PER = LANES // math.gcd(LANES, GX)
TILES = GX // math.gcd(LANES, GX)
HALF = RX // 2
GROUPS = RY // 2 * RX // LANES
LOW = 2 * LANES


def sincos(angle):
    quarter = jnp.round(angle * (2.0 / math.pi))
    rest = angle - quarter * 1.5703125
    rest = rest - quarter * 4.83826794896619e-4
    square = rest * rest
    sine = rest + rest * square * (
        -1.6666654611e-1 + square * (8.3321608736e-3 + square * -1.9515295891e-4)
    )
    cosine = 1.0 - 0.5 * square + square * square * (
        4.166664568298827e-2
        + square * (-1.388731625493765e-3 + square * 2.443315711809948e-5)
    )
    turns = quarter.astype(jnp.int32)
    odd = (turns & 1) == 1
    sin_sign = jnp.where((turns & 2) == 2, -1.0, 1.0)
    cos_sign = jnp.where(((turns + 1) & 2) == 2, -1.0, 1.0)
    return (
        jnp.where(odd, cosine, sine) * sin_sign,
        jnp.where(odd, sine, cosine) * cos_sign,
    )


def prolate(length, count):
    band = math.cos(wave_step)
    at = np.arange(length)
    near = at[1:] * (length - at[1:]) / 2.0
    matrix = np.diag(((length - 1 - 2 * at) / 2.0) ** 2 * band) + np.diag(near, 1) + np.diag(near, -1)
    vectors = np.linalg.eigh(matrix)[1][:, ::-1][:, :count]
    middle = at - (length - 1) / 2.0
    even, odd = vectors[:, 0::2], vectors[:, 1::2]
    even = (even + even[::-1]) / 2.0
    odd = (odd - odd[::-1]) / 2.0
    even = even * np.where(even[length // 2] < 0, -1.0, 1.0)
    odd = odd * np.where(odd[length // 2] < 0, -1.0, 1.0)
    return even, odd


def split(values):
    high = np.asarray(values, np.float32).astype(jnp.bfloat16)
    low = (np.asarray(values, np.float64) - high.astype(np.float64)).astype(np.float32)
    return high, low.astype(jnp.bfloat16)


def tables(cells):
    lines = cells // GX
    tiles = cells // LANES
    even_x, odd_x = prolate(GX, RX)
    even_y, odd_y = prolate(lines, RY)
    both_y = np.stack([even_y, odd_y], axis=2).reshape(lines, RY)
    first = np.zeros((TILES, 2, RY, tiles))
    for tile in range(tiles):
        line = tile * LANES // GX
        for next_line in range(2):
            first[tile % TILES, next_line, :, tile] = both_y[line + next_line]
    first = first.reshape(TILES * 2 * RY, tiles)
    rows = np.concatenate(split(first), axis=1)
    block = np.concatenate([even_x, odd_x], axis=1)
    columns = np.concatenate(split(np.tile(block, (1, LANES // RX))), axis=1)
    pieces = []
    for even, odd in ((even_x, odd_x), (even_y, odd_y)):
        for part in (even, odd):
            length = part.shape[0]
            half = np.zeros((HALF, length // 2))
            half[: part.shape[1]] = 2.0 * part[length // 2 :].T
            pieces.append(half)
    trig = np.stack(pieces)
    high, low = split(trig)
    trig = np.concatenate([high, high, low], axis=2)
    return rows, columns, trig.reshape(4 * HALF, -1)


def high_low(values):
    high = values.astype(BF16)
    return high, (values - high.astype(F32)).astype(BF16)


def kernel(
    slab_size, orient_size, planes, cells_all,
    pol_hbm, occ_hbm, table_hbm, dirs_hbm, rows_hbm, columns_hbm, trig_hbm, out_ref,
    held_pol, held_occ, table_ref, dirs_ref, rows_ref, columns_ref, trig_ref,
    spread, halves, coef, found, turned, vv, landed, mine, parts,
    load_sem, send_sem, recv_sem, part_send, part_recv,
):
    slab = lax.axis_index("slab")
    orient = lax.axis_index("orient")
    is_odd = slab % 2 == 1
    odd = slab + 1 - slab % 2
    width = dirs_ref.shape[2]
    both = 2 * width
    all_orients = table_ref.shape[1]
    tiles = held_occ.shape[0] // planes
    pair_rows = 2 * tiles
    blocks = held_pol.shape[0] // (planes * pair_rows)
    orients = blocks // 3
    group = blocks * 2
    loads = [
        pltpu.make_async_copy(occ_hbm, held_occ, load_sem.at[0]),
        pltpu.make_async_copy(pol_hbm, held_pol, load_sem.at[1]),
        pltpu.make_async_copy(rows_hbm, rows_ref, load_sem.at[2]),
        pltpu.make_async_copy(columns_hbm, columns_ref, load_sem.at[3]),
        pltpu.make_async_copy(dirs_hbm.at[pl.ds(odd - 1, 2)], dirs_ref, load_sem.at[4]),
        pltpu.make_async_copy(table_hbm, table_ref, load_sem.at[5]),
        pltpu.make_async_copy(trig_hbm, trig_ref, load_sem.at[6]),
    ]
    for load in loads:
        load.start()

    barrier = pltpu.get_barrier_semaphore()

    def greet(plane_of, target):
        pl.semaphore_signal(
            barrier, inc=1, device_id=(plane_of, target), device_id_type=MESH
        )

    @pl.when(is_odd)
    def _():
        for step in range(1, slab_size):
            greet(orient, (slab + step) % slab_size)

    @pl.when(jnp.logical_not(is_odd))
    def _():
        greet(orient, odd)

    for step in range(1, orient_size):
        greet((orient + step) % orient_size, odd)

    for load in loads[:4]:
        load.wait()
    lane = lax.broadcasted_iota(jnp.int32, (1, LANES), 1)
    columns = jnp.concatenate([columns_ref[...]] * (2 * PER), axis=0)
    for plane in range(planes):
        kept = held_occ[plane * tiles : (plane + 1) * tiles, :].astype(F32)
        for block in range(blocks):
            at = (block * planes + plane) * pair_rows
            spread[block] = held_pol[at : at + pair_rows, :].astype(F32)
            masked = jnp.concatenate(
                [spread[block, pl.ds(p, tiles, stride=2), :] * kept for p in range(2)], axis=1
            )
            lines = jnp.dot(
                rows_ref[...], jnp.concatenate([masked, masked], axis=0).astype(BF16),
                preferred_element_type=F32,
            )
            stacked = []
            for p in range(2):
                wide = []
                for j in range(TILES):
                    base = j * 2 * RY
                    at = slice(p * LANES, (p + 1) * LANES)
                    limit = GX - j * LANES % GX
                    wide.append(
                        jnp.where(
                            lane < limit,
                            lines[base : base + RY, at],
                            lines[base + RY : base + 2 * RY, at],
                        )
                    )
                stacked.append(jnp.concatenate(wide, axis=1))
            high, low = high_low(jnp.concatenate(stacked, axis=0))
            halves[0, block * 2 * RY : (block + 1) * 2 * RY, :] = high
            halves[1, block * 2 * RY : (block + 1) * 2 * RY, :] = low
        small = jnp.dot(
            jnp.concatenate([halves[0], halves[1]], axis=1), columns,
            preferred_element_type=F32,
        )
        small = small[:, :LANES] + small[:, LANES:]
        coef[0 : group * RY, :] = small
        coef[group * RY : 2 * group * RY, :] = small
        lines_of = [coef[pl.ds(ky, 2 * group, stride=RY), :] for ky in range(RY)]
        upper = lane % RX >= HALF
        is_low = lax.broadcasted_iota(jnp.int32, (2 * group, LANES), 0) >= group
        share_of = LANES // RX
        for g in range(GROUPS):
            picked = []
            for parity in range(2):
                whole = lines_of[2 * (g * share_of + share_of - 1) + parity]
                for q in range(share_of - 2, -1, -1):
                    whole = jnp.where(
                        lane < (q + 1) * RX, lines_of[2 * (g * share_of + q) + parity], whole
                    )
                picked.append(whole)
            for imag in range(2):
                whole = jnp.where(upper, picked[1 - imag], picked[imag])
                high = whole.astype(BF16).astype(F32)
                at = (imag * GROUPS + g) * LANES
                landed[slab, plane, 0 : 2 * group, at : at + LANES] = jnp.where(
                    is_low, whole - high, high
                ).astype(BF16)

    pl.semaphore_wait(barrier, slab_size // 2 + slab % 2 * (2 * orient_size - 2))
    order = list(range(1, slab_size, 2))

    def slab_copy(source, target):
        piece = landed.at[source, :, pl.ds(0, 2 * group), :]
        return pltpu.make_async_remote_copy(
            src_ref=piece,
            dst_ref=piece,
            send_sem=send_sem.at[target],
            recv_sem=recv_sem.at[source],
            device_id=(orient, target),
            device_id_type=MESH,
        )

    for target in order:
        @pl.when(slab != target)
        def _():
            slab_copy(slab, target).start()

    for load in loads[4:]:
        load.wait()

    def part_copy(step, core):
        return pltpu.make_async_remote_copy(
            src_ref=mine.at[core],
            dst_ref=parts.at[orient],
            send_sem=part_send.at[core, step],
            recv_sem=part_recv.at[step],
            device_id=((orient + step) % orient_size, odd - 1 + core),
            device_id_type=MESH,
        )

    routes = [(step, core) for step in range(orient_size - 1, -1, -1) for core in range(2) if step + 1 - core]

    @pl.when(is_odd)
    def _():
        dirs = jnp.concatenate([dirs_ref[0], dirs_ref[1]], axis=1).astype(F32)
        is_polar = lax.broadcasted_iota(jnp.int32, (2, both), 0) == 0
        angles = jnp.where(
            is_polar, (dirs + 0.5) * (math.pi / THETA_GRID), dirs * (2.0 * math.pi / THETA_GRID)
        )
        sines, cosines = sincos(angles)
        sin_p, cos_p = sines[0:1], cosines[0:1]
        sin_a, cos_a = sines[1:2], cosines[1:2]
        azimuth = angles[1:2]
        normals = (sin_p * cos_a, sin_p * sin_a)
        parts_of = []
        for axis in range(2):
            length = trig_ref.shape[1] // 3
            step = lax.broadcasted_iota(jnp.int32, (length, both), 0).astype(F32) + 0.5
            sine, cosine = sincos(step * (wave_step * normals[axis]))
            for kind, wave in enumerate((cosine, sine)):
                high, low = high_low(wave)
                at = (axis * 2 + kind) * HALF
                parts_of.append(
                    jnp.dot(
                        trig_ref[at : at + HALF, :],
                        jnp.concatenate([high, low, high], axis=0),
                        preferred_element_type=F32,
                    )
                )
        even_x, odd_x, even_y, odd_y = parts_of
        deep = RY // 2 * RX
        for a in range(RY // 2):
            one, two = even_y[a : a + 1], odd_y[a : a + 1]
            for kind, pieces in enumerate(
                (
                    (even_x * one, -(odd_x * two)),
                    (even_x * two, odd_x * one),
                )
            ):
                high, low = high_low(jnp.concatenate(pieces, axis=0))
                vv[kind, a * RX : (a + 1) * RX, :] = high
                if a * RX < LOW:
                    vv[kind, deep + a * RX : deep + (a + 1) * RX, :] = low

        tilt_row = lax.broadcasted_iota(jnp.int32, (all_orients, both), 0)
        tilts = jnp.zeros((all_orients, both), F32)
        for o in range(all_orients):
            tilts = jnp.where(tilt_row == o, table_ref[1, o].astype(F32), tilts)
        weights = sincos((tilts + 0.5) * (math.pi / ORIENT_GRID))[0]
        share = 1.0 / (jnp.sum(weights, axis=0, keepdims=True) * cells_all)
        own_row = lax.broadcasted_iota(jnp.int32, (2 * orients, both), 0) % orients
        turns = jnp.zeros((2 * orients, both), F32)
        tilt = jnp.zeros((2 * orients, both), F32)
        for o in range(orients):
            turns = jnp.where(own_row == o, table_ref[0, orient * orients + o].astype(F32), turns)
            tilt = jnp.where(own_row == o, table_ref[1, orient * orients + o].astype(F32), tilt)
        sin_q, cos_q = sincos(azimuth - turns * (2.0 * math.pi / ORIENT_GRID))
        weight = sincos((tilt + 0.5) * (math.pi / ORIENT_GRID))[0] * share
        depth_at = lax.broadcasted_iota(jnp.int32, (slab_size * planes, both), 0).astype(F32)
        sin_z, cos_z = sincos(depth_at * (wave_step * cos_p))
        turned[0] = cos_z
        turned[1] = sin_z

        for source in range(slab_size - 1, -1, -1):
            @pl.when(slab != source)
            def _():
                slab_copy(source, slab).wait_recv()

        space = landed.shape[2]
        everything = landed[...].reshape(slab_size * planes * space, 2 * deep)
        real_in, imag_in = everything[:, :deep], everything[:, deep:]
        real_in = jnp.concatenate([real_in, real_in[:, :LOW]], axis=1)
        imag_in = jnp.concatenate([imag_in, imag_in[:, :LOW]], axis=1)
        piece = min(width, LANES)
        for core in range(2):
            cut = slice(core * width, (core + 1) * width)
            real = jnp.dot(real_in, vv[0, :, cut], preferred_element_type=F32)
            imag = jnp.dot(imag_in, vv[1, :, cut], preferred_element_type=F32)
            total_r = total_i = None
            for z in range(slab_size * planes):
                at = slice(z * space, z * space + 2 * group)
                c, s = turned[0, z : z + 1, cut], turned[1, z : z + 1, cut]
                now_r = real[at] * c - imag[at] * s
                now_i = imag[at] * c + real[at] * s
                total_r = now_r if total_r is None else total_r + now_r
                total_i = now_i if total_i is None else total_i + now_i
            total_r = total_r[:group] + total_r[group:]
            total_i = total_i[:group] + total_i[group:]
            count = width // piece
            for h in range(count):
                found[core * count + h, :group, :piece] = total_r[:, h * piece : (h + 1) * piece]
                found[core * count + h, group:, :piece] = total_i[:, h * piece : (h + 1) * piece]

            def entry(c, p):
                return jnp.concatenate(
                    [
                        found[core * count + h, pl.ds(2 * c + p, 2 * orients, stride=6), :][:, :piece]
                        for h in range(count)
                    ],
                    axis=1,
                )

            par, across = [], []
            for p in range(2):
                one, two, three = entry(0, p), entry(1, p), entry(2, p)
                turned_one = one * cos_q[:, cut] + two * sin_q[:, cut]
                par.append(cos_p[:, cut] * turned_one - sin_p[:, cut] * three)
                across.append(two * cos_q[:, cut] - one * sin_q[:, cut])
            par_square = par[0] * par[0] + par[1] * par[1]
            across_square = across[0] * across[0] + across[1] * across[1]

            def swap(values):
                return jnp.concatenate([values[orients:], -values[:orients]], axis=0)

            elements = (
                0.5 * (par_square + across_square),
                0.5 * (par_square - across_square),
                across[1] * par[0] + across[0] * par[1],
                par[0] * swap(across[1]) + par[1] * swap(across[0]),
            )
            result = jnp.concatenate(
                [jnp.sum(element * weight[:, cut], axis=0, keepdims=True) for element in elements],
                axis=0,
            )
            if core == 0:
                mine[0] = result
            else:
                mine[1] = result
                parts[orient] = result
            for step, target_core in routes:
                if target_core == core:
                    part_copy(step, core).start()

    for target in order:
        @pl.when(slab != target)
        def _():
            slab_copy(slab, target).wait_send()

    def arrival(step):
        back = (orient + orient_size - step) % orient_size
        return pltpu.make_async_remote_copy(
            src_ref=mine.at[0],
            dst_ref=parts.at[back],
            send_sem=part_send.at[0, step],
            recv_sem=part_recv.at[step],
            device_id=(back, odd),
            device_id_type=MESH,
        )

    @pl.when(jnp.logical_not(is_odd))
    def _():
        arrival(0).wait_recv()

    for step in range(1, orient_size):
        arrival(step).wait_recv()
    summed = parts[0]
    for o in range(1, orient_size):
        summed = summed + parts[o]
    out_ref[...] = summed

    @pl.when(is_odd)
    def _():
        for step, core in routes:
            part_copy(step, core).wait_send()


def shards(slab_size, orient_size, polarization, occupied, orient_table, dir_index):
    orients, _, components, planes, cells = polarization.shape
    group = orients * 6
    tiles = cells // LANES
    width = dir_index.shape[0] // slab_size
    pol = polarization.reshape(orients, 2, components, planes, tiles, LANES)
    pol = pol.transpose(0, 2, 3, 4, 1, 5).reshape(-1, LANES)
    occ = occupied.reshape(planes * tiles, LANES)
    dirs = dir_index.T.reshape(2, slab_size, width).transpose(1, 0, 2)
    rows, columns, trig = (jnp.asarray(table) for table in tables(cells))
    space = -(-2 * group // 16) * 16
    deep = RY // 2 * RX
    vmem = pl.BlockSpec(memory_space=pltpu.VMEM)
    anywhere = pl.BlockSpec(memory_space=pltpu.HBM)
    return pl.pallas_call(
        functools.partial(
            kernel, slab_size, orient_size, planes, float(planes * slab_size * cells)
        ),
        out_shape=pltpu.VMEM((4, width), F32),
        in_specs=[anywhere] * 7,
        out_specs=vmem,
        scratch_shapes=[
            pltpu.VMEM(pol.shape, BF16),
            pltpu.VMEM(occ.shape, jnp.int32),
            pltpu.SMEM((2, orient_table.shape[0]), jnp.int32),
            pltpu.VMEM((2, 2, width), jnp.int32),
            pltpu.VMEM(rows.shape, BF16),
            pltpu.VMEM(columns.shape, BF16),
            pltpu.VMEM(trig.shape, BF16),
            pltpu.VMEM((3 * orients, tiles * 2, LANES), F32),
            pltpu.VMEM((2, group * RY, TILES * LANES), BF16),
            pltpu.VMEM((2 * group * RY, LANES), F32),
            pltpu.VMEM((2 * max(width // LANES, 1), 2 * group, LANES), F32),
            pltpu.VMEM((2, slab_size * planes, 2 * width), F32),
            pltpu.VMEM((2, deep + LOW, 2 * width), BF16),
            pltpu.VMEM((slab_size, planes, space, 2 * deep), BF16),
            pltpu.VMEM((2, 4, width), F32),
            pltpu.VMEM((orient_size, 4, width), F32),
            pltpu.SemaphoreType.DMA((7,)),
            pltpu.SemaphoreType.DMA((slab_size,)),
            pltpu.SemaphoreType.DMA((slab_size,)),
            pltpu.SemaphoreType.DMA((2, orient_size)),
            pltpu.SemaphoreType.DMA((orient_size,)),
        ],
        compiler_params=pltpu.CompilerParams(
            collective_id=0, has_side_effects=True
        ),
    )(pol, occ, orient_table.T, dirs, rows, columns, trig)


def solution(mesh):
    return jax.shard_map(
        functools.partial(shards, mesh.shape["slab"], mesh.shape["orient"]),
        mesh=mesh,
        in_specs=(P("orient", None, None, "slab", None), P("slab", None), P(), P()),
        out_specs=P(None, "slab"),
        check_vma=False,
    )
```
